256 devices in a mesh: grp: 8 (over x_hi, y), row: 32 (over z, x_lo, core).
Axes of the slice: x: 4 (x_hi: 2, x_lo: 2; x = x_hi * 2 + x_lo), y: 4, z: 8, core: 2. Of those that a mesh axis runs over, the one named last changes fastest.
Arguments:
- tables: bfloat16 [8, 32768, 512], P(None, 'row', 'grp'), may hold values from -1.1953125 to 1.1953125
- indices: int32 [4096, 8, 32], P('row', 'grp'), may hold values from 0 to 32767
- block_shift: int32 [8], replicated, may hold values from 0 to 31
- pooled_grad: bfloat16 [4096, 8, 512], P('row', 'grp'), may hold values from -6 to 6
Outputs:
- pooled: bfloat16 [4096, 8, 512], P('row', 'grp')
- updated: bfloat16 [8, 32768, 512], P('grp', 'row')
The draws below stay inside these ranges and needn't reach their ends.
All inputs are finite; a program needn't handle non-finite values.
Results may differ from the reference program's by a relative error of at most 0.001.
Values may be sent and summed in bfloat16 or wider, within the bound.
No kernel may reach another device: no remote copies, remote signals or barrier semaphores. Data moves between devices by JAX's collectives and lax.ppermute only.
A program may use at most 64 MiB of HBM per device.

```python
import jax
import jax.numpy as jnp
from jax import lax

DIM = 512
ROWS = 32768
BAG = 32
TABLES = 8
BATCH = 4096
N_ROW = 32


def place_ends(values, own_key, smallest, top_value):
    place = [jax.random.randint(jax.random.fold_in(own_key, axis), (), 0, length) for axis, length in enumerate(values.shape)]
    main_axis = values.shape.index(max(values.shape))
    beside = place[:main_axis] + [(place[main_axis] + 1) % values.shape[main_axis]] + place[main_axis + 1:]
    return values.at[tuple(place)].set(smallest).at[tuple(beside)].set(top_value)


def block_scale(own_key, dims, split, least, top_value):
    level, own = 1.0, jax.random.fold_in(own_key, 6)
    for position, shards_of in split:
        heights = jnp.exp(jax.random.uniform(jax.random.fold_in(own, position), (shards_of,), jnp.float32, least / len(split), top_value / len(split)))
        level = level * jnp.repeat(heights, dims[position] // shards_of).reshape([-1 if axis == position else 1 for axis in range(len(dims))])
    return level


def normal_values(stream_key, dims, spread, limit, cuts=(), kind=jnp.bfloat16):
    drawn = jax.random.normal(stream_key, dims, jnp.float32) * spread
    if len(cuts) > 0:
        drawn = block_scale(stream_key, dims, cuts, -0.22, 0.18) * drawn
    return jnp.clip(drawn, min=-limit, max=limit).astype(kind)


def setup_inputs(seed: int = 0) -> dict:
    splits = jax.random.split(jax.random.key(seed), 5)
    tables = normal_values(splits[0], (TABLES, ROWS, DIM), 0.2, 1.1953125, ((1, 32), (2, 8)))
    indices = place_ends(jax.random.randint(splits[1], (BATCH, TABLES, BAG), 0, ROWS), jax.random.fold_in(splits[1], 1), 0, ROWS - 1).astype(jnp.int32)
    block_shift = place_ends(jax.random.randint(splits[2], (TABLES,), 0, N_ROW), jax.random.fold_in(splits[2], 1), 0, N_ROW - 1).astype(jnp.int32)
    pooled_grad = normal_values(splits[3], (BATCH, TABLES, DIM), 1.0, 6.0, ((0, 32), (1, 8)))
    return {"tables": tables, "indices": indices, "block_shift": block_shift, "pooled_grad": pooled_grad}


step_rate = 0.25


def reference(tables, indices, block_shift, pooled_grad):
    block_rows = ROWS // N_ROW

    def per_table(bundle):
        table_rows, lookups, offset_blocks, upstream = bundle
        gathered = jnp.take(table_rows, lookups, axis=0).astype(jnp.float32)
        pooled = jnp.sum(gathered, axis=1).astype(jnp.bfloat16)
        repeated = jnp.broadcast_to(upstream.astype(jnp.float32)[:, None, :], (BATCH, BAG, DIM)).reshape(BATCH * BAG, DIM)
        gradient = jax.ops.segment_sum(repeated, lookups.reshape(-1), num_segments=ROWS)
        updated = (table_rows.astype(jnp.float32) - step_rate * gradient).astype(jnp.bfloat16)
        rotated = jnp.roll(updated, offset_blocks * block_rows, axis=0)
        return pooled, rotated

    pooled, rotated = lax.map(per_table, (tables, jnp.transpose(indices, (1, 0, 2)), block_shift, jnp.transpose(pooled_grad, (1, 0, 2))))
    return jnp.transpose(pooled, (1, 0, 2)), rotated
```

```python
import jax
import jax.numpy as jnp
from jax import lax
from jax.experimental import pallas as pl
from jax.experimental.pallas import tpu as pltpu
from jax.sharding import Mesh, PartitionSpec as P

STEP_RATE = 0.25
ROW = ("z", "xl", "core")
BLOCK = 1024
PIECE = 32
WINDOW = 256
STATIC_HITS = 4


def count_kernel(keys_ref, out_ref, hits_ref):
    window = pl.program_id(1)
    bag = keys_ref.shape[0]
    empty = jnp.full(keys_ref.shape[1:], -1, jnp.int32)
    hits = []
    total = jnp.zeros(keys_ref.shape[1:], jnp.int32)
    for k in range(bag):
        key = keys_ref[k]
        mine = (key >> 8) == window
        hits.append(empty)
        for j in range(k, 0, -1):
            hits[j] = jnp.where(mine, hits[j - 1], hits[j])
        hits[0] = jnp.where(mine, key & 255, hits[0])
        total = total + jnp.where(mine, 1, 0)
    for j in range(bag):
        hits_ref[j] = hits[j].astype(jnp.float32)
    most = jnp.max(total)
    rows = lax.broadcasted_iota(jnp.int32, (WINDOW, 128), 0).astype(jnp.bfloat16)
    one = jnp.ones((WINDOW, 128), jnp.bfloat16)
    zero = jnp.zeros((WINDOW, 128), jnp.bfloat16)

    def marks(j, d):
        wanted = jnp.broadcast_to(hits_ref[j, pl.ds(d, 1), :], (WINDOW, 128)).astype(jnp.bfloat16)
        return jnp.where(rows == wanted, one, zero)

    for d in range(keys_ref.shape[1]):
        counts = marks(0, d)
        for j in range(1, STATIC_HITS):
            counts = counts + marks(j, d)
        out_ref[:, d * 128 : (d + 1) * 128] = counts

    def more(j, carry):
        for d in range(keys_ref.shape[1]):
            out_ref[:, d * 128 : (d + 1) * 128] += marks(j, d)
        return carry

    lax.fori_loop(STATIC_HITS, most, more, 0)


def count_lookups(keys, rows):
    bag, owners, lanes = keys.shape
    groups = owners // 8
    return pl.pallas_call(
        count_kernel,
        grid=(groups, rows // WINDOW),
        in_specs=[pl.BlockSpec((bag, 8, lanes), lambda g, w: (0, g, 0))],
        out_specs=pl.BlockSpec((WINDOW, 8 * lanes), lambda g, w: (w, g)),
        out_shape=jax.ShapeDtypeStruct((rows, owners * lanes), jnp.bfloat16),
        scratch_shapes=[pltpu.VMEM((bag, 8, lanes), jnp.float32)],
        name="count_lookups",
    )(keys)


def pool_kernel(t0, t1, t2, t3, w_ref, out_ref):
    total = jnp.dot(t0[...], w_ref[0:BLOCK, :], preferred_element_type=jnp.float32)
    for q, t in enumerate((t1, t2, t3), 1):
        total += jnp.dot(t[...], w_ref[q * BLOCK : (q + 1) * BLOCK, :], preferred_element_type=jnp.float32)
    for half in range(2):
        out_ref[half] = total[:, half * 128 : (half + 1) * 128]


def pool(tables, counts):
    dim = tables[0].shape[0]
    samples = counts.shape[1]
    whole = pl.BlockSpec((dim, BLOCK), lambda n: (0, 0))
    return pl.pallas_call(
        pool_kernel,
        grid=(samples // 256,),
        in_specs=[whole] * 4 + [pl.BlockSpec((4 * BLOCK, 256), lambda n: (0, n))],
        out_specs=pl.BlockSpec((2, dim, 128), lambda n: (n, 0, 0)),
        out_shape=jax.ShapeDtypeStruct((samples // 128, dim, 128), jnp.float32),
        name="pool",
    )(*tables, counts)


def per_device(tables, indices, block_shift, pooled_grad):
    z, xl, core = (lax.axis_index(a) for a in ROW)
    me = 4 * z + 2 * xl + core
    shift = lax.dynamic_index_in_dim(block_shift, lax.axis_index("grp"), keepdims=False)
    swap = [(0, 1), (1, 0)]

    grads = lax.all_gather(pooled_grad[:, 0, :], ROW, axis=0, tiled=True)

    columns = lax.all_to_all(jnp.swapaxes(tables, 1, 2), "grp", 0, 0, tiled=True).reshape(-1, BLOCK)

    ids = indices[:, 0, :].T.astype(jnp.int16)
    ids = lax.all_to_all(jnp.broadcast_to(ids, (32,) + ids.shape), ROW, 0, 0, tiled=True)
    ids = jnp.swapaxes(ids.astype(jnp.int32), 0, 1)

    mine = lax.dynamic_index_in_dim(ids.reshape(32, 8, 4, 128), 2 * xl + core, axis=2, keepdims=False)
    near = ((mine >> 10) & 3) ^ (2 * xl + core)
    pool_keys = jnp.where((mine >> 12) == z, (near << 10) | (mine & 1023), -1)
    pool_counts = count_lookups(pool_keys, 4 * BLOCK)
    across_core = lax.ppermute(columns, "core", swap)
    across_xl = lax.ppermute(columns, "xl", swap)
    across_both = lax.ppermute(across_xl, "core", swap)
    partial = pool((columns, across_core, across_xl, across_both), pool_counts)
    pooled = lax.psum_scatter(partial, "z", scatter_dimension=0, tiled=True)[0]
    pooled = pooled.T.astype(jnp.bfloat16)[:, None, :]

    pieces = lax.all_to_all(columns.T.reshape(32, PIECE, -1), ROW, 0, 0, tiled=True)
    pieces = jnp.roll(pieces, shift, axis=0).reshape(BLOCK, -1)
    place = ((ids >> 10) + shift) & 31
    update_keys = jnp.where(((ids >> 5) & 31) == me, (place << 5) | (ids & 31), -1)
    update_counts = count_lookups(update_keys, BLOCK)
    gradient = jnp.dot(update_counts, grads, preferred_element_type=jnp.float32)
    fresh = (pieces.astype(jnp.float32) - STEP_RATE * gradient).astype(jnp.bfloat16)
    updated = lax.all_to_all(fresh.reshape(32, PIECE, -1), ROW, 0, 0, tiled=True)
    return pooled, updated.reshape(1, BLOCK, -1)


def solution(mesh):
    split = Mesh(mesh.devices.reshape(8, 8, 2, 2), ("grp",) + ROW)
    return jax.shard_map(
        per_device,
        mesh=split,
        in_specs=(P(None, ROW, "grp"), P(ROW, "grp", None), P(), P(ROW, "grp", None)),
        out_specs=(P(ROW, "grp", None), P("grp", ROW, None)),
        check_vma=False,
    )
```

```python
import functools

import jax
import jax.numpy as jnp
from jax import lax
from jax.experimental import pallas as pl
from jax.experimental.pallas import tpu as pltpu
from jax.sharding import Mesh, PartitionSpec as P


STEP_RATE = 0.25
ROW = ("z", "xl", "core")
BLOCK = 1024
PIECE = 32
WINDOW = 256
STATIC_HITS = 4
RING_ORDER = (4, 5, 3, 6, 2, 7, 1, 0)


def count_kernel(first_window, keys_ref, out_ref, hits_ref):
    window = first_window + pl.program_id(1)
    bag = keys_ref.shape[0]
    empty = jnp.full(keys_ref.shape[1:], -1, jnp.int32)
    hits = []
    total = jnp.zeros(keys_ref.shape[1:], jnp.int32)
    for k in range(bag):
        key = keys_ref[k]
        mine = (key >> 8) == window
        hits.append(empty)
        for j in range(k, 0, -1):
            hits[j] = jnp.where(mine, hits[j - 1], hits[j])
        hits[0] = jnp.where(mine, key & 255, hits[0])
        total = total + jnp.where(mine, 1, 0)
    for j in range(bag):
        hits_ref[j] = hits[j].astype(jnp.float32)
    most = jnp.max(total)
    rows = lax.broadcasted_iota(jnp.int32, (WINDOW, 128), 0).astype(jnp.bfloat16)
    one = jnp.ones((WINDOW, 128), jnp.bfloat16)
    zero = jnp.zeros((WINDOW, 128), jnp.bfloat16)

    def marks(j, d):
        wanted = jnp.broadcast_to(hits_ref[j, pl.ds(d, 1), :], (WINDOW, 128)).astype(jnp.bfloat16)
        return jnp.where(rows == wanted, one, zero)

    for d in range(keys_ref.shape[1]):
        counts = marks(0, d)
        for j in range(1, STATIC_HITS):
            counts = counts + marks(j, d)
        out_ref[:, d * 128 : (d + 1) * 128] = counts

    def more(j, carry):
        for d in range(keys_ref.shape[1]):
            out_ref[:, d * 128 : (d + 1) * 128] += marks(j, d)
        return carry

    lax.fori_loop(STATIC_HITS, most, more, 0)


def count_lookups(keys, first_row, rows):
    bag, owners, lanes = keys.shape
    groups = owners // 8
    return pl.pallas_call(
        functools.partial(count_kernel, first_row // WINDOW),
        grid=(groups, rows // WINDOW),
        in_specs=[pl.BlockSpec((bag, 8, lanes), lambda g, w: (0, g, 0))],
        out_specs=pl.BlockSpec((WINDOW, 8 * lanes), lambda g, w: (w, g)),
        out_shape=jax.ShapeDtypeStruct((rows, owners * lanes), jnp.bfloat16),
        scratch_shapes=[pltpu.VMEM((bag, 8, lanes), jnp.float32)],
        name="count_lookups",
    )(keys)


def pool_first_kernel(t0, t1, w_ref, out_ref):
    total = jnp.dot(t0[...], w_ref[0:BLOCK, :], preferred_element_type=jnp.float32)
    total += jnp.dot(t1[...], w_ref[BLOCK:, :], preferred_element_type=jnp.float32)
    for half in range(2):
        out_ref[half] = total[:, half * 128 : (half + 1) * 128]


def pool_first(t0, t1, counts):
    dim = t0.shape[0]
    samples = counts.shape[1]
    whole = pl.BlockSpec((dim, BLOCK), lambda n: (0, 0))
    return pl.pallas_call(
        pool_first_kernel,
        grid=(samples // 256,),
        in_specs=[whole] * 2 + [pl.BlockSpec((2 * BLOCK, 256), lambda n: (0, n))],
        out_specs=pl.BlockSpec((2, dim, 128), lambda n: (n, 0, 0)),
        out_shape=jax.ShapeDtypeStruct((samples // 128, dim, 128), jnp.float32),
        name="pool_first",
    )(t0, t1, counts)


def pool_rest_kernel(t0, t1, w_ref, first_ref, left_ref, right_ref):
    total = jnp.dot(t0[...], w_ref[0:BLOCK, :], preferred_element_type=jnp.float32)
    total += jnp.dot(t1[...], w_ref[BLOCK:, :], preferred_element_type=jnp.float32)
    left_ref[...] = total[:, :128] + first_ref[0]
    right_ref[...] = total[:, 128:] + first_ref[1]


def pool_rest(t0, t1, counts, first, pair):
    dim = t0.shape[0]
    whole = pl.BlockSpec((dim, BLOCK), lambda n: (0, 0))
    result = jax.ShapeDtypeStruct((dim, 128), jnp.float32)
    return pl.pallas_call(
        pool_rest_kernel,
        grid=(1,),
        in_specs=[whole] * 2
        + [pl.BlockSpec((2 * BLOCK, 256), lambda n: (0, pair)), pl.BlockSpec((2, dim, 128), lambda n: (pair, 0, 0))],
        out_specs=[pl.BlockSpec((dim, 128), lambda n: (0, 0))] * 2,
        out_shape=[result, result],
        name="pool_rest",
    )(t0, t1, counts, first)


def update_kernel(shift_ref, w0, w1, g0, g1, pieces_ref, out_ref):
    step = pl.program_id(0)
    gradient = jnp.dot(w0[...], g0[...], preferred_element_type=jnp.float32)
    gradient += jnp.dot(w1[...], g1[...], preferred_element_type=jnp.float32)
    for i in range(out_ref.shape[0]):
        old = pieces_ref[(8 * step + i - shift_ref[0]) & 31].astype(jnp.float32)
        out_ref[i] = (old - STEP_RATE * gradient[i * PIECE : (i + 1) * PIECE]).astype(jnp.bfloat16)


def update(shift, counts, grads, pieces):
    rows, samples = counts[0].shape
    dim = grads[0].shape[1]
    return pl.pallas_call(
        update_kernel,
        grid_spec=pltpu.PrefetchScalarGridSpec(
            num_scalar_prefetch=1,
            grid=(rows // 256,),
            in_specs=[pl.BlockSpec((256, samples), lambda n, s: (n, 0))] * 2
            + [pl.BlockSpec((samples, dim), lambda n, s: (0, 0))] * 2
            + [pl.BlockSpec(pieces.shape, lambda n, s: (0, 0, 0))],
            out_specs=pl.BlockSpec((8, PIECE, dim), lambda n, s: (n, 0, 0)),
        ),
        out_shape=jax.ShapeDtypeStruct(pieces.shape, jnp.bfloat16),
        name="update",
    )(shift, *counts, *grads, pieces)


def swap(values, axis):
    return lax.ppermute(values, axis, [(0, 1), (1, 0)])


def pass_on(values, by):
    return lax.ppermute(values, "z", [(i, (i + by) % 8) for i in range(8)])


def step(tables, indices, block_shift, pooled_grad):
    z, xl, core = (lax.axis_index(a) for a in ROW)
    quarter = 2 * xl + core
    shift = lax.dynamic_slice_in_dim(block_shift, lax.axis_index("grp"), 1)

    columns = lax.all_to_all(jnp.swapaxes(tables, 1, 2), "grp", 0, 0, tiled=True).reshape(-1, BLOCK)

    own = pooled_grad[:, 0, :]
    own = jnp.concatenate([own, swap(own, "xl")], axis=0)
    up, down = [own], [own]
    for hop in range(1, 5):
        up.append(pass_on(up[-1], 1))
        if hop < 4:
            down.append(pass_on(down[-1], -1))
    own_grads = jnp.concatenate(up + down[:0:-1], axis=0)
    other_grads = swap(own_grads, "core")

    ids = indices[:, 0, :].T.astype(jnp.int16)
    ids = lax.all_to_all(jnp.broadcast_to(ids, (8,) + ids.shape), "z", 0, 0, tiled=True)
    ids = lax.dynamic_slice_in_dim(jnp.concatenate([ids[::-1]] * 2, axis=0), 7 - z, 8)
    ids = ids[None]
    beside = swap(ids, "xl")
    ids_both = jnp.concatenate([ids, beside], axis=0)
    ids_other = swap(ids_both, "core")

    mine = ids[0].astype(jnp.int32)
    near = ((mine >> 10) & 3) ^ quarter
    pool_keys = jnp.where((mine >> 12) == z, (near << 10) | (mine & 1023), -1)
    pool_keys = jnp.stack([pool_keys[i] for i in RING_ORDER], axis=1)
    counts_near = count_lookups(pool_keys, 0, 2 * BLOCK)
    counts_far = count_lookups(pool_keys, 2 * BLOCK, 2 * BLOCK)
    across_core = swap(columns, "core")
    across_xl = swap(columns, "xl")
    across_both = swap(across_xl, "core")
    first = pool_first(columns, across_core, counts_near)
    sums = [None] * 8
    for pair in range(4):
        left, right = pool_rest(across_xl, across_both, counts_far, first, pair)
        sums[RING_ORDER[2 * pair]], sums[RING_ORDER[2 * pair + 1]] = left, right
    lower, upper = sums[4], sums[5]
    for hop in range(1, 5):
        lower = pass_on(lower, -1) + sums[4 - hop]
        if hop < 4:
            upper = pass_on(upper, 1)
            if hop < 3:
                upper = upper + sums[5 + hop]
    pooled = (lower + upper).T.astype(jnp.bfloat16)[:, None, :]

    pieces = lax.all_to_all(columns.T.reshape(32, PIECE, -1), ROW, 0, 0, tiled=True)
    counts = []
    for looked_up in (ids_both, ids_other):
        looked_up = looked_up.astype(jnp.int32).transpose(2, 1, 0, 3).reshape(32, 16, 128)
        place = ((looked_up >> 10) + shift[0]) & 31
        keys = jnp.where(((looked_up >> 5) & 31) == 4 * z + quarter, (place << 5) | (looked_up & 31), -1)
        counts.append(count_lookups(keys, 0, BLOCK))
    fresh = update(shift, counts, (own_grads, other_grads), pieces)
    updated = lax.all_to_all(fresh, ROW, 0, 0, tiled=True)
    return pooled, updated.reshape(1, BLOCK, -1)


def solution(mesh):
    split = Mesh(mesh.devices.reshape(8, 8, 2, 2), ("grp",) + ROW)
    return jax.shard_map(
        step,
        mesh=split,
        in_specs=(P(None, ROW, "grp"), P(ROW, "grp", None), P(), P(ROW, "grp", None)),
        out_specs=(P(ROW, "grp", None), P("grp", ROW, None)),
        check_vma=False,
    )
```

```python
import jax
import jax.numpy as jnp
from jax import lax
from jax.experimental import pallas as pl
from jax.experimental.pallas import tpu as pltpu
from jax.sharding import Mesh, PartitionSpec as P


STEP_RATE = 0.25
ROW = ("z", "xl", "core")
BLOCK = 1024
PIECE = 32
WINDOW = 256
STATIC_HITS = 4


def count_kernel(keys_ref, out_ref, hits_ref):
    windows = out_ref.shape[1] // WINDOW
    bag, owners, lanes = keys_ref.shape
    most = jnp.zeros((owners, lanes), jnp.int32)
    for w in range(windows):
        window = pl.program_id(1) * windows + w
        hits = []
        total = jnp.zeros((owners, lanes), jnp.int32)
        for k in range(bag):
            key = keys_ref[k]
            mine = (key >> 8) == window
            hits.append(jnp.full((owners, lanes), -1, jnp.int32))
            for j in range(k, 0, -1):
                hits[j] = jnp.where(mine, hits[j - 1], hits[j])
            hits[0] = jnp.where(mine, key & 255, hits[0])
            total = total + jnp.where(mine, 1, 0)
        for j in range(bag):
            hits_ref[w, j] = hits[j].astype(jnp.float32)
        most = jnp.maximum(most, total)
    rows = lax.broadcasted_iota(jnp.int32, (WINDOW, lanes), 0).astype(jnp.bfloat16)
    one = jnp.ones((WINDOW, lanes), jnp.bfloat16)
    zero = jnp.zeros((WINDOW, lanes), jnp.bfloat16)

    def marks(w, j, d):
        wanted = jnp.broadcast_to(hits_ref[w, j, pl.ds(d, 1), :], (WINDOW, lanes)).astype(jnp.bfloat16)
        return jnp.where(rows == wanted, one, zero)

    def place(w, d):
        return d, pl.ds(w * WINDOW, WINDOW)

    for w in range(windows):
        for d in range(owners):
            counts = marks(w, 0, d)
            for j in range(1, STATIC_HITS):
                counts = counts + marks(w, j, d)
            out_ref[place(w, d)] = counts

    def more(j, carry):
        for w in range(windows):
            for d in range(owners):
                out_ref[place(w, d)] += marks(w, j, d)
        return carry

    lax.fori_loop(STATIC_HITS, jnp.max(most), more, 0)


def count_lookups(keys, rows):
    bag, owners, lanes = keys.shape
    return pl.pallas_call(
        count_kernel,
        grid=(owners // 8, rows // BLOCK),
        in_specs=[pl.BlockSpec((bag, 8, lanes), lambda g, w: (0, g, 0))],
        out_specs=pl.BlockSpec((8, BLOCK, lanes), lambda g, w: (g, w, 0)),
        out_shape=jax.ShapeDtypeStruct((owners, rows, lanes), jnp.bfloat16),
        scratch_shapes=[pltpu.VMEM((BLOCK // WINDOW, bag, 8, lanes), jnp.float32)],
        name="count",
    )(keys)


def side_by_side(w_ref, rows=slice(None)):
    return jnp.concatenate([w_ref[i, rows] for i in range(w_ref.shape[0])], axis=1)


def pool_kernel(t0, t1, t2, t3, w_ref, out_ref):
    total = jnp.dot(t0[...], side_by_side(w_ref, slice(0, BLOCK)), preferred_element_type=jnp.float32)
    for q, t in enumerate((t1, t2, t3), 1):
        rows = slice(q * BLOCK, (q + 1) * BLOCK)
        total += jnp.dot(t[...], side_by_side(w_ref, rows), preferred_element_type=jnp.float32)
    for half in range(2):
        out_ref[half] = total[:, half * 128 : (half + 1) * 128]


def pool(tables, counts):
    dim = tables[0].shape[0]
    owners, rows, lanes = counts.shape
    return pl.pallas_call(
        pool_kernel,
        grid=(owners // 2,),
        in_specs=[pl.BlockSpec((dim, BLOCK), lambda n: (0, 0))] * 4
        + [pl.BlockSpec((2, rows, lanes), lambda n: (n, 0, 0))],
        out_specs=pl.BlockSpec((2, dim, lanes), lambda n: (n, 0, 0)),
        out_shape=jax.ShapeDtypeStruct((owners, dim, lanes), jnp.float32),
        name="pool",
    )(*tables, counts)


def update_kernel(shift_ref, w_ref, grads_ref, pieces_ref, out_ref):
    step = pl.program_id(0)
    gradient = jnp.dot(side_by_side(w_ref), grads_ref[...], preferred_element_type=jnp.float32)
    for i in range(out_ref.shape[0]):
        old = pieces_ref[(8 * step + i - shift_ref[0]) & 31].astype(jnp.float32)
        out_ref[i] = (old - STEP_RATE * gradient[i * PIECE : (i + 1) * PIECE]).astype(jnp.bfloat16)


def update(shift, counts, grads, pieces):
    owners, rows, lanes = counts.shape
    samples, dim = grads.shape
    return pl.pallas_call(
        update_kernel,
        grid_spec=pltpu.PrefetchScalarGridSpec(
            num_scalar_prefetch=1,
            grid=(rows // 256,),
            in_specs=[
                pl.BlockSpec((owners, 256, lanes), lambda n, s: (0, n, 0)),
                pl.BlockSpec((samples, dim), lambda n, s: (0, 0)),
                pl.BlockSpec(pieces.shape, lambda n, s: (0, 0, 0)),
            ],
            out_specs=pl.BlockSpec((8, PIECE, dim), lambda n, s: (n, 0, 0)),
        ),
        out_shape=jax.ShapeDtypeStruct(pieces.shape, jnp.bfloat16),
        name="update",
    )(shift, counts, grads, pieces)


def swap(values, axis):
    return lax.ppermute(values, axis, [(0, 1), (1, 0)])


def step(tables, indices, block_shift, pooled_grad):
    z, xl, core = (lax.axis_index(a) for a in ROW)
    quarter = 2 * xl + core
    shift = lax.dynamic_slice_in_dim(block_shift, lax.axis_index("grp"), 1)

    own = pooled_grad[:, 0, :]
    own = jnp.concatenate([own, swap(own, "xl")], axis=0)
    grads = lax.all_gather(own, ("z", "core"), axis=0, tiled=True)

    columns = lax.all_to_all(jnp.swapaxes(tables, 1, 2), "grp", 0, 0, tiled=True).reshape(-1, BLOCK)

    ids = indices[:, 0, :].T.astype(jnp.int16)[None]
    ids = jnp.concatenate([ids, swap(ids, "xl")], axis=0)
    beside = swap(ids, "core")
    ids = jnp.where(core == 0, jnp.stack([ids, beside]), jnp.stack([beside, ids]))
    below = [ids]
    for hop in range(1, 8):
        below.append(lax.ppermute(ids, "z", [(i, (i + hop) % 8) for i in range(8)]))
    ids = jnp.stack(below[::-1] * 2)
    ids = lax.dynamic_slice_in_dim(ids, 7 - z, 8).astype(jnp.int32)

    mine = lax.dynamic_index_in_dim(ids[:, :, 0], core, axis=1, keepdims=False).swapaxes(0, 1)
    near = ((mine >> 10) & 3) ^ quarter
    pool_keys = jnp.where((mine >> 12) == z, (near << 10) | (mine & 1023), -1)
    pool_counts = count_lookups(pool_keys, 4 * BLOCK)
    across_core = swap(columns, "core")
    across_xl = swap(columns, "xl")
    across_both = swap(across_xl, "core")
    partial = pool((columns, across_core, across_xl, across_both), pool_counts)
    pooled = lax.psum_scatter(partial, "z", scatter_dimension=0, tiled=True)[0]
    pooled = pooled.T.astype(jnp.bfloat16)[:, None, :]

    pieces = lax.all_to_all(columns.T.reshape(32, PIECE, -1), ROW, 0, 0, tiled=True)
    lookups = ids.transpose(3, 0, 1, 2, 4).reshape(32, 32, 128)
    place = ((lookups >> 10) + shift[0]) & 31
    keys = jnp.where(((lookups >> 5) & 31) == 4 * z + quarter, (place << 5) | (lookups & 31), -1)
    counts = count_lookups(keys, BLOCK)
    fresh = update(shift, counts, grads, pieces)
    updated = lax.all_to_all(fresh, ROW, 0, 0, tiled=True)
    return pooled, updated.reshape(1, BLOCK, -1)


def solution(mesh):
    split = Mesh(mesh.devices.reshape(8, 8, 2, 2), ("grp",) + ROW)
    return jax.shard_map(
        step,
        mesh=split,
        in_specs=(P(None, ROW, "grp"), P(ROW, "grp", None), P(), P(ROW, "grp", None)),
        out_specs=(P(ROW, "grp", None), P("grp", ROW, None)),
        check_vma=False,
    )
```

```python
import jax
import jax.numpy as jnp
from jax import lax
from jax.experimental import pallas as pl
from jax.experimental.pallas import tpu as pltpu
from jax.sharding import Mesh, PartitionSpec as P


STEP_RATE = 0.25
ROW = ("z", "xl", "core")
BLOCK = 1024
PIECE = 32
WINDOW = 256
STATIC_HITS = 4


def count_kernel(keys_ref, out_ref, hits_ref):
    windows = out_ref.shape[1] // WINDOW
    bag, owners, lanes = keys_ref.shape
    most = jnp.zeros((owners, lanes), jnp.int32)
    for w in range(windows):
        window = pl.program_id(1) * windows + w
        hits = []
        total = jnp.zeros((owners, lanes), jnp.int32)
        for k in range(bag):
            key = keys_ref[k]
            mine = (key >> 8) == window
            hits.append(jnp.full((owners, lanes), -1, jnp.int32))
            for j in range(k, 0, -1):
                hits[j] = jnp.where(mine, hits[j - 1], hits[j])
            hits[0] = jnp.where(mine, key & 255, hits[0])
            total = total + jnp.where(mine, 1, 0)
        for j in range(bag):
            hits_ref[w, j] = hits[j].astype(jnp.float32)
        most = jnp.maximum(most, total)
    rows = lax.broadcasted_iota(jnp.int32, (WINDOW, lanes), 0).astype(jnp.bfloat16)
    one = jnp.ones((WINDOW, lanes), jnp.bfloat16)
    zero = jnp.zeros((WINDOW, lanes), jnp.bfloat16)

    def marks(w, j, d):
        wanted = jnp.broadcast_to(hits_ref[w, j, pl.ds(d, 1), :], (WINDOW, lanes)).astype(jnp.bfloat16)
        return jnp.where(rows == wanted, one, zero)

    def place(w, d):
        return d, pl.ds(w * WINDOW, WINDOW)

    for w in range(windows):
        for d in range(owners):
            counts = marks(w, 0, d)
            for j in range(1, STATIC_HITS):
                counts = counts + marks(w, j, d)
            out_ref[place(w, d)] = counts

    def more(j, carry):
        for w in range(windows):
            for d in range(owners):
                out_ref[place(w, d)] += marks(w, j, d)
        return carry

    lax.fori_loop(STATIC_HITS, jnp.max(most), more, 0)


def count_lookups(keys, rows):
    bag, owners, lanes = keys.shape
    return pl.pallas_call(
        count_kernel,
        grid=(owners // 8, rows // BLOCK),
        in_specs=[pl.BlockSpec((bag, 8, lanes), lambda g, w: (0, g, 0))],
        out_specs=pl.BlockSpec((8, BLOCK, lanes), lambda g, w: (g, w, 0)),
        out_shape=jax.ShapeDtypeStruct((owners, rows, lanes), jnp.bfloat16),
        scratch_shapes=[pltpu.VMEM((BLOCK // WINDOW, bag, 8, lanes), jnp.float32)],
        name="count",
    )(keys)


def side_by_side(w_ref, rows=slice(None)):
    return jnp.concatenate([w_ref[i, rows] for i in range(w_ref.shape[0])], axis=1)


def pool_kernel(t0, t1, t2, t3, w_ref, out_ref):
    total = jnp.dot(t0[...], side_by_side(w_ref, slice(0, BLOCK)), preferred_element_type=jnp.float32)
    for q, t in enumerate((t1, t2, t3), 1):
        rows = slice(q * BLOCK, (q + 1) * BLOCK)
        total += jnp.dot(t[...], side_by_side(w_ref, rows), preferred_element_type=jnp.float32)
    for half in range(2):
        out_ref[half] = total[:, half * 128 : (half + 1) * 128]


def pool(tables, counts):
    dim = tables[0].shape[0]
    owners, rows, lanes = counts.shape
    return pl.pallas_call(
        pool_kernel,
        grid=(owners // 2,),
        in_specs=[pl.BlockSpec(memory_space=pltpu.VMEM)] * 4
        + [pl.BlockSpec((2, rows, lanes), lambda n: (n, 0, 0))],
        out_specs=pl.BlockSpec((2, dim, lanes), lambda n: (n, 0, 0)),
        out_shape=jax.ShapeDtypeStruct((owners, dim, lanes), jnp.float32),
        name="pool",
    )(*tables, counts)


def gradient_kernel(w_ref, grads_ref, out_ref):
    out_ref[...] = jnp.dot(side_by_side(w_ref), grads_ref[...], preferred_element_type=jnp.float32)


def row_gradient(counts, grads):
    owners, rows, lanes = counts.shape
    dim = grads.shape[1]
    return pl.pallas_call(
        gradient_kernel,
        grid=(rows // 256,),
        in_specs=[pl.BlockSpec((owners, 256, lanes), lambda n: (0, n, 0)), pl.BlockSpec(grads.shape, lambda n: (0, 0))],
        out_specs=pl.BlockSpec((256, dim), lambda n: (n, 0)),
        out_shape=jax.ShapeDtypeStruct((rows, dim), jnp.float32),
        name="gradient",
    )(counts, grads)


def update_kernel(shift_ref, gradient_ref, pieces_ref, out_ref):
    for i in range(out_ref.shape[0]):
        step = STEP_RATE * gradient_ref[i * PIECE : (i + 1) * PIECE]
        old = pieces_ref[(8 * pl.program_id(0) + i - shift_ref[0]) & 31].astype(jnp.float32)
        out_ref[i] = (old - step).astype(jnp.bfloat16)


def update(shift, gradient, pieces):
    dim = gradient.shape[1]
    return pl.pallas_call(
        update_kernel,
        grid_spec=pltpu.PrefetchScalarGridSpec(
            num_scalar_prefetch=1,
            grid=(4,),
            in_specs=[
                pl.BlockSpec((8 * PIECE, dim), lambda n, s: (n, 0)),
                pl.BlockSpec(memory_space=pltpu.VMEM),
            ],
            out_specs=pl.BlockSpec((8, PIECE, dim), lambda n, s: (n, 0, 0)),
        ),
        out_shape=jax.ShapeDtypeStruct(pieces.shape, jnp.bfloat16),
        name="update",
    )(shift, gradient, pieces)


def swap(values, axis):
    return lax.ppermute(values, axis, [(0, 1), (1, 0)])


def step(tables, indices, block_shift, pooled_grad):
    z, xl, core = (lax.axis_index(a) for a in ROW)
    quarter = 2 * xl + core
    shift = lax.dynamic_slice_in_dim(block_shift, lax.axis_index("grp"), 1)

    own = pooled_grad[:, 0, :]
    own = jnp.concatenate([own, swap(own, "xl")], axis=0)
    grads = lax.all_gather(own, ("z", "core"), axis=0, tiled=True)

    columns = lax.all_to_all(jnp.swapaxes(tables, 1, 2), "grp", 0, 0, tiled=True).reshape(-1, BLOCK)

    mine = indices[:, 0, :].T.astype(jnp.int16)
    mine = lax.all_to_all(jnp.broadcast_to(mine, (8,) + mine.shape), "z", 0, 0, tiled=True)

    lookups = mine.astype(jnp.int32).swapaxes(0, 1)
    near = ((lookups >> 10) & 3) ^ quarter
    pool_keys = jnp.where((lookups >> 12) == z, (near << 10) | (lookups & 1023), -1)
    pool_counts = count_lookups(pool_keys, 4 * BLOCK)
    across_core = swap(columns, "core")
    across_xl = swap(columns, "xl")
    across_both = swap(across_xl, "core")
    partial = pool((columns, across_core, across_xl, across_both), pool_counts)
    pooled = lax.psum_scatter(partial, "z", scatter_dimension=0, tiled=True)[0]
    pooled = pooled.T.astype(jnp.bfloat16)[:, None, :]

    pieces = lax.all_to_all(columns.T.reshape(32, PIECE, -1), ROW, 0, 0, tiled=True)
    both = jnp.stack([mine, swap(mine, "xl")], axis=1)
    beside = swap(both, "core")
    lookups = jnp.where(core == 0, jnp.stack([both, beside], axis=1), jnp.stack([beside, both], axis=1))
    lookups = lookups.astype(jnp.int32).transpose(3, 0, 1, 2, 4).reshape(32, 32, 128)
    place = ((lookups >> 10) + shift[0]) & 31
    keys = jnp.where(((lookups >> 5) & 31) == 4 * z + quarter, (place << 5) | (lookups & 31), -1)
    counts = count_lookups(keys, BLOCK)
    gradient = row_gradient(counts, grads)
    fresh = update(shift, gradient, pieces)
    updated = lax.all_to_all(fresh, ROW, 0, 0, tiled=True)
    return pooled, updated.reshape(1, BLOCK, -1)


def solution(mesh):
    split = Mesh(mesh.devices.reshape(8, 8, 2, 2), ("grp",) + ROW)
    return jax.shard_map(
        step,
        mesh=split,
        in_specs=(P(None, ROW, "grp"), P(ROW, "grp", None), P(), P(ROW, "grp", None)),
        out_specs=(P(ROW, "grp", None), P("grp", ROW, None)),
        check_vma=False,
    )
```

```python
import jax
import jax.numpy as jnp
from jax import lax
from jax.experimental import pallas as pl
from jax.experimental.pallas import tpu as pltpu
from jax.sharding import Mesh, PartitionSpec as P


STEP_RATE = 0.25
ROW = ("z", "xl", "core")
BLOCK = 1024
PIECE = 32
WINDOW = 256
STATIC_HITS = 4


def count_kernel(keys_ref, out_ref, hits_ref):
    windows = out_ref.shape[1] // WINDOW
    bag, owners, lanes = keys_ref.shape
    most = jnp.zeros((owners, lanes), jnp.int32)
    for w in range(windows):
        window = pl.program_id(1) * windows + w
        hits = []
        total = jnp.zeros((owners, lanes), jnp.int32)
        for k in range(bag):
            key = keys_ref[k]
            mine = (key >> 8) == window
            hits.append(jnp.full((owners, lanes), -1, jnp.int32))
            for j in range(k, 0, -1):
                hits[j] = jnp.where(mine, hits[j - 1], hits[j])
            hits[0] = jnp.where(mine, key & 255, hits[0])
            total = total + jnp.where(mine, 1, 0)
        for j in range(bag):
            hits_ref[w, j] = hits[j].astype(jnp.float32)
        most = jnp.maximum(most, total)
    rows = lax.broadcasted_iota(jnp.int32, (WINDOW, lanes), 0).astype(jnp.bfloat16)
    one = jnp.ones((WINDOW, lanes), jnp.bfloat16)
    zero = jnp.zeros((WINDOW, lanes), jnp.bfloat16)

    def marks(w, j, d):
        wanted = jnp.broadcast_to(hits_ref[w, j, pl.ds(d, 1), :], (WINDOW, lanes)).astype(jnp.bfloat16)
        return jnp.where(rows == wanted, one, zero)

    def place(w, d):
        return d, pl.ds(w * WINDOW, WINDOW)

    for w in range(windows):
        for d in range(owners):
            counts = marks(w, 0, d)
            for j in range(1, STATIC_HITS):
                counts = counts + marks(w, j, d)
            out_ref[place(w, d)] = counts

    def more(j, carry):
        for w in range(windows):
            for d in range(owners):
                out_ref[place(w, d)] += marks(w, j, d)
        return carry

    lax.fori_loop(STATIC_HITS, jnp.max(most), more, 0)


def count_lookups(keys, rows):
    bag, owners, lanes = keys.shape
    return pl.pallas_call(
        count_kernel,
        grid=(owners // 8, rows // BLOCK),
        in_specs=[pl.BlockSpec((bag, 8, lanes), lambda g, w: (0, g, 0))],
        out_specs=pl.BlockSpec((8, BLOCK, lanes), lambda g, w: (g, w, 0)),
        out_shape=jax.ShapeDtypeStruct((owners, rows, lanes), jnp.bfloat16),
        scratch_shapes=[pltpu.VMEM((BLOCK // WINDOW, bag, 8, lanes), jnp.float32)],
        name="count",
    )(keys)


def side_by_side(w_ref, rows=slice(None)):
    return jnp.concatenate([w_ref[i, rows] for i in range(w_ref.shape[0])], axis=1)


def pool_kernel(t0, t1, t2, t3, w_ref, out_ref):
    total = jnp.dot(t0[...], side_by_side(w_ref, slice(0, BLOCK)), preferred_element_type=jnp.float32)
    for q, t in enumerate((t1, t2, t3), 1):
        rows = slice(q * BLOCK, (q + 1) * BLOCK)
        total += jnp.dot(t[...], side_by_side(w_ref, rows), preferred_element_type=jnp.float32)
    for half in range(2):
        out_ref[half] = total[:, half * 128 : (half + 1) * 128]


def pool(tables, counts):
    dim = tables[0].shape[0]
    owners, rows, lanes = counts.shape
    return pl.pallas_call(
        pool_kernel,
        grid=(owners // 2,),
        in_specs=[pl.BlockSpec(memory_space=pltpu.VMEM)] * 4
        + [pl.BlockSpec((2, rows, lanes), lambda n: (n, 0, 0))],
        out_specs=pl.BlockSpec((2, dim, lanes), lambda n: (n, 0, 0)),
        out_shape=jax.ShapeDtypeStruct((owners, dim, lanes), jnp.float32),
        name="pool",
    )(*tables, counts)


def update_kernel(shift_ref, w_ref, grads_ref, pieces_ref, out_ref):
    gradient = jnp.dot(side_by_side(w_ref), grads_ref[...], preferred_element_type=jnp.float32)
    for i in range(out_ref.shape[0]):
        old = pieces_ref[(8 * pl.program_id(0) + i - shift_ref[0]) & 31].astype(jnp.float32)
        out_ref[i] = (old - STEP_RATE * gradient[i * PIECE : (i + 1) * PIECE]).astype(jnp.bfloat16)


def update(shift, counts, grads, pieces):
    owners, rows, lanes = counts.shape
    samples, dim = grads.shape
    return pl.pallas_call(
        update_kernel,
        grid_spec=pltpu.PrefetchScalarGridSpec(
            num_scalar_prefetch=1,
            grid=(rows // 256,),
            in_specs=[
                pl.BlockSpec((owners, 256, lanes), lambda n, s: (0, n, 0)),
                pl.BlockSpec((samples, dim), lambda n, s: (0, 0)),
                pl.BlockSpec(pieces.shape, lambda n, s: (0, 0, 0)),
            ],
            out_specs=pl.BlockSpec((8, PIECE, dim), lambda n, s: (n, 0, 0)),
        ),
        out_shape=jax.ShapeDtypeStruct(pieces.shape, jnp.bfloat16),
        name="update",
    )(shift, counts, grads, pieces)


def swap(values, axis):
    return lax.ppermute(values, axis, [(0, 1), (1, 0)])


def step(tables, indices, block_shift, pooled_grad):
    z, xl, core = (lax.axis_index(a) for a in ROW)
    quarter = 2 * xl + core
    shift = lax.dynamic_slice_in_dim(block_shift, lax.axis_index("grp"), 1)

    own = pooled_grad[:, 0, :]
    across = swap(own, "xl")
    own = jnp.concatenate([own, across], axis=0)
    grads = lax.all_gather(own, ("z", "core"), axis=0, tiled=True)

    columns = lax.all_to_all(jnp.swapaxes(tables, 1, 2), "grp", 0, 0, tiled=True).reshape(-1, BLOCK)

    mine = indices[:, 0, :].T.astype(jnp.int16)
    mine = lax.all_to_all(jnp.broadcast_to(mine, (8,) + mine.shape), "z", 0, 0, tiled=True)

    lookups = mine.astype(jnp.int32).swapaxes(0, 1)
    near = ((lookups >> 10) & 3) ^ quarter
    pool_keys = jnp.where((lookups >> 12) == z, (near << 10) | (lookups & 1023), -1)
    pool_counts = count_lookups(pool_keys, 4 * BLOCK)
    across_core = swap(columns, "core")
    across_xl = swap(columns, "xl")
    across_both = swap(across_xl, "core")
    partial = pool((columns, across_core, across_xl, across_both), pool_counts)
    pooled = lax.psum_scatter(partial, "z", scatter_dimension=0, tiled=True)[0]
    pooled = pooled.T.astype(jnp.bfloat16)[:, None, :]

    pieces = lax.all_to_all(columns.T.reshape(32, PIECE, -1), ROW, 0, 0, tiled=True)
    both = jnp.stack([mine, swap(mine, "xl")], axis=1)
    beside = swap(both, "core")
    lookups = jnp.where(core == 0, jnp.stack([both, beside], axis=1), jnp.stack([beside, both], axis=1))
    lookups = lookups.astype(jnp.int32).transpose(3, 0, 1, 2, 4).reshape(32, 32, 128)
    place = ((lookups >> 10) + shift[0]) & 31
    keys = jnp.where(((lookups >> 5) & 31) == 4 * z + quarter, (place << 5) | (lookups & 31), -1)
    counts = count_lookups(keys, BLOCK)
    fresh = update(shift, counts, grads, pieces)
    updated = lax.all_to_all(fresh, ROW, 0, 0, tiled=True)
    return pooled, updated.reshape(1, BLOCK, -1)


def solution(mesh):
    split = Mesh(mesh.devices.reshape(8, 8, 2, 2), ("grp",) + ROW)
    return jax.shard_map(
        step,
        mesh=split,
        in_specs=(P(None, ROW, "grp"), P(ROW, "grp", None), P(), P(ROW, "grp", None)),
        out_specs=(P(ROW, "grp", None), P("grp", ROW, None)),
        check_vma=False,
    )
```

```python
import functools

import jax
import jax.numpy as jnp
from jax import lax
from jax.experimental import pallas as pl
from jax.experimental.pallas import tpu as pltpu
from jax.sharding import Mesh, PartitionSpec as P


STEP_RATE = 0.25
ROW = ("z", "xl", "core")
BLOCK = 1024
PIECE = 32
WINDOW = 256
STATIC_HITS = 4


def pool_key(ids, where_ref):
    near = ((ids >> 10) & 3) ^ where_ref[1]
    return jnp.where((ids >> 12) == where_ref[0], (near << 10) | (ids & 1023), -1)


def update_key(ids, where_ref):
    place = ((ids >> 10) + where_ref[2]) & 31
    return jnp.where(((ids >> 5) & 31) == 4 * where_ref[0] + where_ref[1], (place << 5) | (ids & 31), -1)


def count_kernel(key_of, where_ref, ids_ref, out_ref, keys_ref, hits_ref):
    owners = out_ref.shape[0]
    windows = out_ref.shape[1] // WINDOW
    bag, _, lanes = keys_ref.shape
    for k in range(bag):
        keys_ref[k] = key_of(ids_ref[pl.ds(k, owners, stride=bag), :], where_ref)
    most = jnp.zeros((owners, lanes), jnp.int32)
    for w in range(windows):
        window = pl.program_id(1) * windows + w
        hits = []
        total = jnp.zeros((owners, lanes), jnp.int32)
        for k in range(bag):
            key = keys_ref[k]
            mine = (key >> 8) == window
            hits.append(jnp.full((owners, lanes), -1, jnp.int32))
            for j in range(k, 0, -1):
                hits[j] = jnp.where(mine, hits[j - 1], hits[j])
            hits[0] = jnp.where(mine, key & 255, hits[0])
            total = total + jnp.where(mine, 1, 0)
        for j in range(bag):
            hits_ref[w, j] = hits[j].astype(jnp.float32)
        most = jnp.maximum(most, total)
    rows = lax.broadcasted_iota(jnp.int32, (WINDOW, lanes), 0).astype(jnp.bfloat16)
    one = jnp.ones((WINDOW, lanes), jnp.bfloat16)
    zero = jnp.zeros((WINDOW, lanes), jnp.bfloat16)

    def marks(w, j, d):
        wanted = jnp.broadcast_to(hits_ref[w, j, pl.ds(d, 1), :], (WINDOW, lanes)).astype(jnp.bfloat16)
        return jnp.where(rows == wanted, one, zero)

    def place(w, d):
        return d, pl.ds(w * WINDOW, WINDOW)

    for w in range(windows):
        for d in range(owners):
            counts = marks(w, 0, d)
            for j in range(1, STATIC_HITS):
                counts = counts + marks(w, j, d)
            out_ref[place(w, d)] = counts

    def more(j, carry):
        for w in range(windows):
            for d in range(owners):
                out_ref[place(w, d)] += marks(w, j, d)
        return carry

    lax.fori_loop(STATIC_HITS, jnp.max(most), more, 0)


def count_lookups(key_of, where, ids, rows):
    owners, bag, lanes = ids.shape
    return pl.pallas_call(
        functools.partial(count_kernel, key_of),
        grid_spec=pltpu.PrefetchScalarGridSpec(
            num_scalar_prefetch=1,
            grid=(owners // 8, rows // BLOCK),
            in_specs=[pl.BlockSpec((8 * bag, lanes), lambda g, w, s: (g, 0))],
            out_specs=pl.BlockSpec((8, BLOCK, lanes), lambda g, w, s: (g, w, 0)),
            scratch_shapes=[
                pltpu.VMEM((bag, 8, lanes), jnp.int32),
                pltpu.VMEM((BLOCK // WINDOW, bag, 8, lanes), jnp.float32),
            ],
        ),
        out_shape=jax.ShapeDtypeStruct((owners, rows, lanes), jnp.bfloat16),
        name="count",
    )(where, ids.reshape(owners * bag, lanes))


def side_by_side(w_ref, rows=slice(None)):
    return jnp.concatenate([w_ref[i, rows] for i in range(w_ref.shape[0])], axis=1)


def pool_kernel(where_ref, t0, t1, t2, t3, w_ref, out_ref):
    total = jnp.dot(t0[...], side_by_side(w_ref, slice(0, BLOCK)), preferred_element_type=jnp.float32)
    for q, t in enumerate((t1, t2, t3), 1):
        rows = slice(q * BLOCK, (q + 1) * BLOCK)
        total += jnp.dot(t[...], side_by_side(w_ref, rows), preferred_element_type=jnp.float32)
    for half in range(2):
        out_ref[half ^ (where_ref[0] & 1)] = total[:, half * 128 : (half + 1) * 128]


def pool(where, tables, counts):
    dim = tables[0].shape[0]
    owners, rows, lanes = counts.shape
    return pl.pallas_call(
        pool_kernel,
        grid_spec=pltpu.PrefetchScalarGridSpec(
            num_scalar_prefetch=1,
            grid=(owners // 2,),
            in_specs=[pl.BlockSpec(memory_space=pltpu.VMEM)] * 4
            + [pl.BlockSpec((2, rows, lanes), lambda n, s: (n, 0, 0))],
            out_specs=pl.BlockSpec((2, dim, lanes), lambda n, s: ((s[0] >> 1) ^ n, 0, 0)),
        ),
        out_shape=jax.ShapeDtypeStruct((owners, dim, lanes), jnp.float32),
        name="pool",
    )(where, *tables, counts)


def class_gradient(where_ref, w_ref, *grads):
    total = None
    for core, g in enumerate(grads):
        counts = jnp.concatenate([w_ref[core * 8 + (z ^ where_ref[0])] for z in range(8)], axis=1)
        part = jnp.dot(counts, g[...], preferred_element_type=jnp.float32)
        total = part if total is None else total + part
    return total


def gradient_kernel(where_ref, w_ref, g0, g1, out_ref):
    out_ref[...] = class_gradient(where_ref, w_ref, g0, g1)


def update_kernel(where_ref, w_ref, g0, g1, before_ref, pieces_ref, out_ref):
    gradient = before_ref[...] + class_gradient(where_ref, w_ref, g0, g1)
    for i in range(out_ref.shape[0]):
        old = pieces_ref[(8 * pl.program_id(0) + i - where_ref[2]) & 31].astype(jnp.float32)
        out_ref[i] = (old - STEP_RATE * gradient[i * PIECE : (i + 1) * PIECE]).astype(jnp.bfloat16)


def apply_counts(where, counts, grads, *more):
    owners, rows, lanes = counts.shape
    dim = grads[0].shape[1]
    tile = pl.BlockSpec((256, dim), lambda n, s: (n, 0))
    specs = [pl.BlockSpec((owners, 256, lanes), lambda n, s: (0, n, 0))]
    specs += [pl.BlockSpec(g.shape, lambda n, s: (0, 0)) for g in grads]
    if more:
        specs += [tile, pl.BlockSpec(more[1].shape, lambda n, s: (0, 0, 0))]
        out_spec = pl.BlockSpec((8, PIECE, dim), lambda n, s: (n, 0, 0))
        out_shape = jax.ShapeDtypeStruct(more[1].shape, jnp.bfloat16)
    else:
        out_spec, out_shape = tile, jax.ShapeDtypeStruct((rows, dim), jnp.float32)
    return pl.pallas_call(
        update_kernel if more else gradient_kernel,
        grid_spec=pltpu.PrefetchScalarGridSpec(
            num_scalar_prefetch=1, grid=(rows // 256,), in_specs=specs, out_specs=out_spec
        ),
        out_shape=out_shape,
        name="update" if more else "gradient",
    )(where, counts, *grads, *more)


def swap(values, axis):
    return lax.ppermute(values, axis, [(0, 1), (1, 0)])


def step(tables, indices, block_shift, pooled_grad):
    z, xl, core = (lax.axis_index(a) for a in ROW)
    shift = lax.dynamic_index_in_dim(block_shift, lax.axis_index("grp"), keepdims=False)
    where = jnp.stack([z, 2 * xl + core, shift])

    grads = lax.all_gather(pooled_grad[:, 0, :], "z", axis=0, tiled=True)

    columns = lax.all_to_all(jnp.swapaxes(tables, 1, 2), "grp", 0, 0, tiled=True).reshape(-1, BLOCK)

    ids = indices[:, 0, :].T.astype(jnp.int16)[None]
    for hop in (1, 2, 4):
        arrived = lax.ppermute(ids, "z", [(i, i ^ hop) for i in range(8)])
        ids = jnp.concatenate([ids, arrived], axis=0)
    ids = ids.astype(jnp.int32)
    both = jnp.concatenate([ids, swap(ids, "core")], axis=0)
    both_across = swap(both, "xl")

    pool_counts = count_lookups(pool_key, where, ids, 4 * BLOCK)
    across_core = swap(columns, "core")
    across_xl = swap(columns, "xl")
    across_both = swap(across_xl, "core")
    partial = pool(where, (columns, across_core, across_xl, across_both), pool_counts)
    pooled = lax.psum_scatter(partial, "z", scatter_dimension=0, tiled=True)[0]
    pooled = pooled.T.astype(jnp.bfloat16)[:, None, :]

    pieces = lax.all_to_all(columns.T.reshape(32, PIECE, -1), ROW, 0, 0, tiled=True)
    counts_own = count_lookups(update_key, where, both, BLOCK)
    counts_across = count_lookups(update_key, where, both_across, BLOCK)
    gradient = apply_counts(where, counts_own, (grads, swap(grads, "core")))
    grads = swap(grads, "xl")
    fresh = apply_counts(where, counts_across, (grads, swap(grads, "core")), gradient, pieces)
    updated = lax.all_to_all(fresh, ROW, 0, 0, tiled=True)
    return pooled, updated.reshape(1, BLOCK, -1)


def solution(mesh):
    split = Mesh(mesh.devices.reshape(8, 8, 2, 2), ("grp",) + ROW)
    return jax.shard_map(
        step,
        mesh=split,
        in_specs=(P(None, ROW, "grp"), P(ROW, "grp", None), P(), P(ROW, "grp", None)),
        out_specs=(P(ROW, "grp", None), P("grp", ROW, None)),
        check_vma=False,
    )
```

```python
import functools

import jax
import jax.numpy as jnp
from jax import lax
from jax.experimental import pallas as pl
from jax.experimental.pallas import tpu as pltpu
from jax.sharding import Mesh, PartitionSpec as P


STEP_RATE = 0.25
ROW = ("z", "xl", "core")
BLOCK = 1024
PIECE = 32
WINDOW = 256
STATIC_HITS = 4


def pool_key(ids, where_ref):
    near = ((ids >> 10) & 3) ^ where_ref[1]
    return jnp.where((ids >> 12) == where_ref[0], (near << 10) | (ids & 1023), -1)


def update_key(ids, where_ref):
    place = ((ids >> 10) + where_ref[2]) & 31
    return jnp.where(((ids >> 5) & 31) == 4 * where_ref[0] + where_ref[1], (place << 5) | (ids & 31), -1)


def count_kernel(key_of, where_ref, ids_ref, out_ref, keys_ref, hits_ref):
    owners = out_ref.shape[0]
    windows = out_ref.shape[1] // WINDOW
    bag, _, lanes = keys_ref.shape
    for k in range(bag):
        keys_ref[k] = key_of(ids_ref[pl.ds(k, owners, stride=bag), :], where_ref)
    most = jnp.zeros((owners, lanes), jnp.int32)
    for w in range(windows):
        window = pl.program_id(1) * windows + w
        hits = []
        total = jnp.zeros((owners, lanes), jnp.int32)
        for k in range(bag):
            key = keys_ref[k]
            mine = (key >> 8) == window
            hits.append(jnp.full((owners, lanes), -1, jnp.int32))
            for j in range(k, 0, -1):
                hits[j] = jnp.where(mine, hits[j - 1], hits[j])
            hits[0] = jnp.where(mine, key & 255, hits[0])
            total = total + jnp.where(mine, 1, 0)
        for j in range(bag):
            hits_ref[w, j] = hits[j].astype(jnp.float32)
        most = jnp.maximum(most, total)
    rows = lax.broadcasted_iota(jnp.int32, (WINDOW, lanes), 0).astype(jnp.bfloat16)
    one = jnp.ones((WINDOW, lanes), jnp.bfloat16)
    zero = jnp.zeros((WINDOW, lanes), jnp.bfloat16)

    def marks(w, j, d):
        wanted = jnp.broadcast_to(hits_ref[w, j, pl.ds(d, 1), :], (WINDOW, lanes)).astype(jnp.bfloat16)
        return jnp.where(rows == wanted, one, zero)

    def place(w, d):
        return d, pl.ds(w * WINDOW, WINDOW)

    for w in range(windows):
        for d in range(owners):
            counts = marks(w, 0, d)
            for j in range(1, STATIC_HITS):
                counts = counts + marks(w, j, d)
            out_ref[place(w, d)] = counts

    def more(j, carry):
        for w in range(windows):
            for d in range(owners):
                out_ref[place(w, d)] += marks(w, j, d)
        return carry

    lax.fori_loop(STATIC_HITS, jnp.max(most), more, 0)


def count_lookups(key_of, where, ids, rows):
    owners, bag, lanes = ids.shape
    return pl.pallas_call(
        functools.partial(count_kernel, key_of),
        grid_spec=pltpu.PrefetchScalarGridSpec(
            num_scalar_prefetch=1,
            grid=(owners // 8, rows // BLOCK),
            in_specs=[pl.BlockSpec((8 * bag, lanes), lambda g, w, s: (g, 0))],
            out_specs=pl.BlockSpec((8, BLOCK, lanes), lambda g, w, s: (g, w, 0)),
            scratch_shapes=[
                pltpu.VMEM((bag, 8, lanes), jnp.int32),
                pltpu.VMEM((BLOCK // WINDOW, bag, 8, lanes), jnp.float32),
            ],
        ),
        out_shape=jax.ShapeDtypeStruct((owners, rows, lanes), jnp.bfloat16),
        name="count",
    )(where, ids.reshape(owners * bag, lanes))


def side_by_side(w_ref, rows=slice(None)):
    return jnp.concatenate([w_ref[i, rows] for i in range(w_ref.shape[0])], axis=1)


def pool_kernel(where_ref, t0, t1, t2, t3, w_ref, out_ref):
    total = jnp.dot(t0[...], side_by_side(w_ref, slice(0, BLOCK)), preferred_element_type=jnp.float32)
    for q, t in enumerate((t1, t2, t3), 1):
        rows = slice(q * BLOCK, (q + 1) * BLOCK)
        total += jnp.dot(t[...], side_by_side(w_ref, rows), preferred_element_type=jnp.float32)
    for half in range(2):
        out_ref[half ^ (where_ref[0] & 1)] = total[:, half * 128 : (half + 1) * 128]


def pool(where, tables, counts):
    dim = tables[0].shape[0]
    owners, rows, lanes = counts.shape
    return pl.pallas_call(
        pool_kernel,
        grid_spec=pltpu.PrefetchScalarGridSpec(
            num_scalar_prefetch=1,
            grid=(owners // 2,),
            in_specs=[pl.BlockSpec(memory_space=pltpu.VMEM)] * 4
            + [pl.BlockSpec((2, rows, lanes), lambda n, s: (n, 0, 0))],
            out_specs=pl.BlockSpec((2, dim, lanes), lambda n, s: ((s[0] >> 1) ^ n, 0, 0)),
        ),
        out_shape=jax.ShapeDtypeStruct((owners, dim, lanes), jnp.float32),
        name="pool",
    )(where, *tables, counts)


def update_kernel(where_ref, w_own, w_across, grads_ref, pieces_ref, out_ref):
    order = [((c ^ (where_ref[1] & 1)) * 8 + (z ^ where_ref[0])) for z in range(8) for c in range(2)]
    counts = jnp.concatenate([w[i] for i in order for w in (w_own, w_across)], axis=1)
    gradient = jnp.dot(counts, grads_ref[...], preferred_element_type=jnp.float32)
    for i in range(out_ref.shape[0]):
        old = pieces_ref[(8 * pl.program_id(0) + i - where_ref[2]) & 31].astype(jnp.float32)
        out_ref[i] = (old - STEP_RATE * gradient[i * PIECE : (i + 1) * PIECE]).astype(jnp.bfloat16)


def update(where, counts, grads, pieces):
    owners, rows, lanes = counts[0].shape
    dim = grads.shape[1]
    return pl.pallas_call(
        update_kernel,
        grid_spec=pltpu.PrefetchScalarGridSpec(
            num_scalar_prefetch=1,
            grid=(rows // 256,),
            in_specs=[pl.BlockSpec((owners, 256, lanes), lambda n, s: (0, n, 0))] * 2
            + [pl.BlockSpec(grads.shape, lambda n, s: (0, 0)), pl.BlockSpec(pieces.shape, lambda n, s: (0, 0, 0))],
            out_specs=pl.BlockSpec((8, PIECE, dim), lambda n, s: (n, 0, 0)),
        ),
        out_shape=jax.ShapeDtypeStruct(pieces.shape, jnp.bfloat16),
        name="update",
    )(where, *counts, grads, pieces)


def swap(values, axis):
    return lax.ppermute(values, axis, [(0, 1), (1, 0)])


def step(tables, indices, block_shift, pooled_grad):
    z, xl, core = (lax.axis_index(a) for a in ROW)
    shift = lax.dynamic_index_in_dim(block_shift, lax.axis_index("grp"), keepdims=False)
    where = jnp.stack([z, 2 * xl + core, shift])

    own = pooled_grad[:, 0, :]
    across = swap(own, "xl")
    own = jnp.concatenate([own, across], axis=0)
    grads = lax.all_gather(own, ("z", "core"), axis=0, tiled=True)

    columns = lax.all_to_all(jnp.swapaxes(tables, 1, 2), "grp", 0, 0, tiled=True).reshape(-1, BLOCK)

    ids = indices[:, 0, :].T.astype(jnp.int16)[None]
    for hop in (1, 2, 4):
        arrived = lax.ppermute(ids, "z", [(i, i ^ hop) for i in range(8)])
        ids = jnp.concatenate([ids, arrived], axis=0)
    ids = ids.astype(jnp.int32)
    both = jnp.concatenate([ids, swap(ids, "core")], axis=0)
    both_across = swap(both, "xl")

    pool_counts = count_lookups(pool_key, where, ids, 4 * BLOCK)
    across_core = swap(columns, "core")
    across_xl = swap(columns, "xl")
    across_both = swap(across_xl, "core")
    partial = pool(where, (columns, across_core, across_xl, across_both), pool_counts)
    pooled = lax.psum_scatter(partial, "z", scatter_dimension=0, tiled=True)[0]
    pooled = pooled.T.astype(jnp.bfloat16)[:, None, :]

    pieces = lax.all_to_all(columns.T.reshape(32, PIECE, -1), ROW, 0, 0, tiled=True)
    counts_own = count_lookups(update_key, where, both, BLOCK)
    counts_across = count_lookups(update_key, where, both_across, BLOCK)
    fresh = update(where, (counts_own, counts_across), grads, pieces)
    updated = lax.all_to_all(fresh, ROW, 0, 0, tiled=True)
    return pooled, updated.reshape(1, BLOCK, -1)


def solution(mesh):
    split = Mesh(mesh.devices.reshape(8, 8, 2, 2), ("grp",) + ROW)
    return jax.shard_map(
        step,
        mesh=split,
        in_specs=(P(None, ROW, "grp"), P(ROW, "grp", None), P(), P(ROW, "grp", None)),
        out_specs=(P(ROW, "grp", None), P("grp", ROW, None)),
        check_vma=False,
    )
```
